32 devices in a mesh: section: 2 (over y), dp: 16 (over z, x, core).
Axes of the slice: x: 2, y: 2, z: 4, core: 2. Of those that a mesh axis runs over, the one named last changes fastest.
Arguments:
- residuals: float32 [8, 128, 4096], P('section', 'dp'), may hold values from -100 to 100, as said below
- owners: int32 [32], replicated, may hold values from 0 to 31, each once
Outputs:
- harvest: bfloat16 [128, 8, 4096], P(('section', 'dp'))
The draws below stay inside these ranges and needn't reach their ends.
Inputs may be any that keep to these rules, and one draw needn't show every extreme that they name: `owners`: a permutation of the block numbers. `residuals`: real-valued activations.
All inputs are finite; a program needn't handle non-finite values.
Results may differ from the reference program's by a relative error of at most 0.0004.
Values may be sent and summed in bfloat16 or wider, within the bound.
No kernel may reach another device: no remote copies, remote signals or barrier semaphores. Data moves between devices by JAX's collectives and lax.ppermute only.
A program may use at most 64 MiB of HBM per device.

```python
import math
import jax
import jax.numpy as jnp
from jax import lax

D = 4096
BLOCK = 4
LAYERS = 8
TOK_DEV = 8
TOKENS = 128
BLOCKS = 32


def draw_residuals(key, part):
    noise_key = jax.random.fold_in(key, 11)
    shard_key = jax.random.fold_in(key, 12)
    token_key = jax.random.fold_in(key, 13)
    offset_key = jax.random.fold_in(key, 14)
    shard_count = TOKENS // TOK_DEV
    base_noise = jax.random.normal(noise_key, (LAYERS, TOKENS, D), jnp.float32)
    log_low = math.log(0.3)
    log_high = math.log(3.0)
    shard_scale = jnp.exp(jax.random.uniform(shard_key, (LAYERS, shard_count, 1, 1), jnp.float32, log_low, log_high))
    token_scale = jax.random.uniform(token_key, (LAYERS, TOKENS, 1), jnp.float32, 0.5, 1.5)
    offset = 2.0 * jax.random.normal(offset_key, (LAYERS, TOKENS, 1), jnp.float32)
    scaled_rows = base_noise.reshape(LAYERS, shard_count, TOK_DEV, D) * shard_scale
    return jnp.clip(scaled_rows.reshape(LAYERS, TOKENS, D) * token_scale + offset, -100.0, 100.0)


def setup_inputs(seed: int = 0) -> dict:
    key_list = jax.random.split(jax.random.key(seed), 3)
    return {
        "residuals": draw_residuals(jax.random.fold_in(key_list[2], 71), 0),
        "owners": jax.random.permutation(key_list[1], BLOCKS).astype(jnp.int32),
    }


def reference(residuals, owners):

    def normalize_layer(layer_rows):
        centered = layer_rows - lax.optimization_barrier(jnp.mean(layer_rows, axis=1, keepdims=True))
        energy = jnp.sum(centered * centered)
        layer_scale = 1.0 / jnp.sqrt(energy / (TOKENS * D) + 1.0)
        return (centered * layer_scale).astype(jnp.bfloat16)
    normed = lax.map(normalize_layer, residuals)
    inverse = jnp.zeros((BLOCKS,), jnp.int32).at[owners.astype(jnp.int32)].set(jnp.arange(BLOCKS, dtype=jnp.int32))
    blocked = normed.reshape(LAYERS, BLOCKS, BLOCK, D)[:, inverse]
    return blocked.transpose(1, 2, 0, 3).reshape(TOKENS, LAYERS, D)
```

```python
import jax
import jax.numpy as jnp
from jax import lax
from jax.experimental import pallas as pl
from jax.experimental.pallas import tpu as pltpu
from jax.sharding import PartitionSpec as P

LANES = 128
SUBLANES = 8


def spread_kernel(x_ref, out_ref):
    layer_dev, tok_dev, features = x_ref.shape
    groups = out_ref.shape[0]
    strips = features // groups // LANES
    rows = tok_dev * layer_dev
    row_layer = lax.broadcasted_iota(jnp.int32, (SUBLANES, LANES), 0) % layer_dev
    energy = jnp.zeros((SUBLANES, LANES), jnp.float32)
    for layer in range(layer_dev):
        value = x_ref[layer]
        centered = value - jnp.mean(value, axis=1, keepdims=True)
        partial_value = jnp.sum(centered * centered)
        energy = jnp.where(row_layer == layer, partial_value, energy)
        for strip in range(groups * strips):
            group, part = divmod(strip, strips)
            out_ref[group, pl.ds(part * rows + layer, tok_dev, stride=layer_dev), :] = centered[
                :, strip * LANES : (strip + 1) * LANES
            ]
    for group in range(groups):
        out_ref[group, strips * rows :, :] = energy


def route_kernel(count, block_rows, owners_ref, x_ref, out_ref):
    groups, all_rows, _ = x_ref.shape
    blocks, message_rows, _ = out_ref.shape
    strips = message_rows // block_rows
    rows = (all_rows - SUBLANES) // strips
    blocks_dev = blocks // groups
    energy = x_ref[0, strips * rows :, :]
    for group in range(1, groups):
        energy += x_ref[group, strips * rows :, :]
    scale = 1.0 / jnp.sqrt(energy / count + 1.0)
    scale = jnp.concatenate([scale] * (block_rows // SUBLANES), axis=0)
    for group in range(groups):
        for block in range(blocks_dev):
            owner = owners_ref[group * blocks_dev + block]
            for part in range(strips):
                start = part * rows + block * block_rows
                value = x_ref[group, start : start + block_rows, :] * scale
                out_ref[owner, part * block_rows : (part + 1) * block_rows, :] = value.astype(
                    jnp.bfloat16
                )


def merge_kernel(layer_dev, x_ref, out_ref):
    block_len, layers, features = out_ref.shape
    devices, message_rows, _ = x_ref.shape
    block_rows = block_len * layer_dev
    strips = message_rows // block_rows
    sections = layers // layer_dev
    groups = devices // sections
    for group in range(groups):
        for part in range(strips):
            column = (group * strips + part) * LANES
            for token in range(block_len):
                start = part * block_rows + token * layer_dev
                value = jnp.concatenate(
                    [
                        x_ref[section * groups + group, start : start + layer_dev, :]
                        for section in range(sections)
                    ],
                    axis=0,
                )
                out_ref[token, :, column : column + LANES] = value


def on_device(residuals, owners):
    layer_dev, tok_dev, features = residuals.shape
    groups = lax.axis_size("dp")
    sections = lax.axis_size("section")
    blocks = owners.shape[0]
    block_len = tok_dev * groups // blocks
    strips = features // groups // LANES
    rows = tok_dev * layer_dev
    block_rows = block_len * layer_dev
    message = pl.pallas_call(
        spread_kernel,
        out_shape=jax.ShapeDtypeStruct((groups, strips * rows + SUBLANES, LANES), jnp.float32),
        name="spread",
    )(residuals)
    spread = lax.all_to_all(message, "dp", split_axis=0, concat_axis=0, tiled=True)
    routed = pl.pallas_call(
        lambda *refs: route_kernel(float(tok_dev * groups * features), block_rows, *refs),
        out_shape=jax.ShapeDtypeStruct((blocks, strips * block_rows, LANES), jnp.bfloat16),
        in_specs=[
            pl.BlockSpec(memory_space=pltpu.SMEM),
            pl.BlockSpec(memory_space=pltpu.VMEM),
        ],
        name="route",
    )(owners, spread)
    received = lax.all_to_all(routed, ("section", "dp"), split_axis=0, concat_axis=0, tiled=True)
    return pl.pallas_call(
        lambda *refs: merge_kernel(layer_dev, *refs),
        out_shape=jax.ShapeDtypeStruct((block_len, layer_dev * sections, features), jnp.bfloat16),
        name="merge",
    )(received)


def solution(mesh):
    in_specs = (P("section", "dp", None), P())
    out_specs = P(("section", "dp"), None, None)
    return jax.shard_map(
        on_device, mesh=mesh, in_specs=in_specs, out_specs=out_specs, check_vma=False
    )
```

```python
import jax
import jax.numpy as jnp
from jax import lax
from jax.experimental import pallas as pl
from jax.experimental.pallas import tpu as pltpu
from jax.sharding import PartitionSpec as P

LANES = 128
SUBLANES = 8
LOCAL = pltpu.CompilerParams(vmem_limit_bytes=16 * 1024 * 1024)


def spread_kernel(x_ref, out_ref):
    layer_dev, tok_dev, features = x_ref.shape
    groups = out_ref.shape[0]
    strips = features // groups // LANES
    rows = tok_dev * layer_dev
    row_layer = lax.broadcasted_iota(jnp.int32, (SUBLANES, LANES), 0) % layer_dev
    energy = jnp.zeros((SUBLANES, LANES), jnp.float32)
    for layer in range(layer_dev):
        value = x_ref[layer]
        centered = value - jnp.mean(value, axis=1, keepdims=True)
        partial_value = jnp.sum(centered * centered)
        energy = jnp.where(row_layer == layer, partial_value, energy)
        for strip in range(groups * strips):
            group, part = divmod(strip, strips)
            out_ref[group, pl.ds(part * rows + layer, tok_dev, stride=layer_dev), :] = centered[
                :, strip * LANES : (strip + 1) * LANES
            ]
    for group in range(groups):
        out_ref[group, strips * rows :, :] = energy


def route_kernel(count, block_rows, owners_ref, x_ref, out_ref):
    groups, all_rows, _ = x_ref.shape
    blocks, message_rows, _ = out_ref.shape
    strips = message_rows // block_rows
    rows = (all_rows - SUBLANES) // strips
    blocks_dev = blocks // groups
    energy = x_ref[0, strips * rows :, :]
    for group in range(1, groups):
        energy += x_ref[group, strips * rows :, :]
    scale = 1.0 / jnp.sqrt(energy / count + 1.0)
    scale = jnp.concatenate([scale] * (block_rows // SUBLANES), axis=0)
    for group in range(groups):
        for block in range(blocks_dev):
            owner = owners_ref[group * blocks_dev + block]
            for part in range(strips):
                start = part * rows + block * block_rows
                value = x_ref[group, start : start + block_rows, :] * scale
                out_ref[owner, part * block_rows : (part + 1) * block_rows, :] = value.astype(
                    jnp.bfloat16
                )


def merge_kernel(layer_dev, x_ref, out_ref):
    block_len, layers, features = out_ref.shape
    devices, message_rows, _ = x_ref.shape
    block_rows = block_len * layer_dev
    strips = message_rows // block_rows
    sections = layers // layer_dev
    groups = devices // sections
    for group in range(groups):
        for part in range(strips):
            column = (group * strips + part) * LANES
            for token in range(block_len):
                start = part * block_rows + token * layer_dev
                value = jnp.concatenate(
                    [
                        x_ref[section * groups + group, start : start + layer_dev, :]
                        for section in range(sections)
                    ],
                    axis=0,
                )
                out_ref[token, :, column : column + LANES] = value


def on_device(residuals, owners):
    layer_dev, tok_dev, features = residuals.shape
    groups = lax.axis_size("dp")
    sections = lax.axis_size("section")
    blocks = owners.shape[0]
    block_len = tok_dev * groups // blocks
    strips = features // groups // LANES
    rows = tok_dev * layer_dev
    block_rows = block_len * layer_dev
    message = pl.pallas_call(
        spread_kernel,
        out_shape=jax.ShapeDtypeStruct((groups, strips * rows + SUBLANES, LANES), jnp.float32),
        compiler_params=LOCAL,
        name="spread",
    )(residuals)
    spread = lax.all_to_all(message, "dp", split_axis=0, concat_axis=0, tiled=True)
    routed = pl.pallas_call(
        lambda *refs: route_kernel(float(tok_dev * groups * features), block_rows, *refs),
        out_shape=jax.ShapeDtypeStruct((blocks, strips * block_rows, LANES), jnp.bfloat16),
        in_specs=[
            pl.BlockSpec(memory_space=pltpu.SMEM),
            pl.BlockSpec(memory_space=pltpu.VMEM),
        ],
        compiler_params=LOCAL,
        name="route",
    )(owners, spread)
    received = lax.all_to_all(routed, ("section", "dp"), split_axis=0, concat_axis=0, tiled=True)
    return pl.pallas_call(
        lambda *refs: merge_kernel(layer_dev, *refs),
        out_shape=jax.ShapeDtypeStruct((block_len, layer_dev * sections, features), jnp.bfloat16),
        compiler_params=LOCAL,
        name="merge",
    )(received)


def solution(mesh):
    in_specs = (P("section", "dp", None), P())
    out_specs = P(("section", "dp"), None, None)
    return jax.shard_map(
        on_device, mesh=mesh, in_specs=in_specs, out_specs=out_specs, check_vma=False
    )
```

```python
import jax
import jax.numpy as jnp
from jax import lax
from jax.experimental import pallas as pl
from jax.experimental.pallas import tpu as pltpu
from jax.sharding import PartitionSpec as P

LANES = 128
SUBLANES = 8
PARTS = 3
LOCAL = pltpu.CompilerParams(vmem_limit_bytes=16 * 1024 * 1024)


def split(value):
    high = value.astype(jnp.bfloat16)
    return high, value - high.astype(jnp.float32)


def energy_slots(shape, layer_dev):
    row = lax.broadcasted_iota(jnp.int32, shape, 0)
    lane = lax.broadcasted_iota(jnp.int32, shape, 1)
    return row, lane, (row < layer_dev) & (lane < PARTS)


def spread_kernel(x_ref, out_ref, rows_ref):
    layer_dev, tok_dev, features = x_ref.shape
    groups, all_rows, _ = out_ref.shape
    strips = features // groups // LANES
    rows = tok_dev * layer_dev
    half = all_rows // 2
    tile = 2 * SUBLANES
    row, lane, slots = energy_slots((tile, LANES), layer_dev)
    energy = jnp.zeros((tile, LANES), jnp.float32)
    for layer in range(layer_dev):
        value = x_ref[layer]
        centered = value - jnp.mean(value, axis=1, keepdims=True)
        energy = jnp.where(row == layer, jnp.sum(centered * centered), energy)
        for strip in range(groups * strips):
            rows_ref[pl.ds(strip * rows + layer, tok_dev, stride=layer_dev), :] = centered[
                :, strip * LANES : (strip + 1) * LANES
            ]
    first, rest = split(energy)
    second, rest = split(rest)
    energy = jnp.where(lane == 0, first.astype(jnp.float32), jnp.where(lane == 1, second.astype(jnp.float32), rest))
    for group in range(groups):
        for start in range(0, half, tile):
            high, rest = split(rows_ref[group * half + start : group * half + start + tile, :])
            if start == half - tile:
                rest = jnp.where(slots, energy, rest)
            out_ref[group, start : start + tile, :] = high
            out_ref[group, half + start : half + start + tile, :] = rest.astype(jnp.bfloat16)


def route_kernel(count, layer_dev, block_rows, owners_ref, x_ref, out_ref):
    groups, all_rows, _ = x_ref.shape
    blocks, message_rows, _ = out_ref.shape
    strips = message_rows // block_rows
    half = all_rows // 2
    rows = half // strips
    blocks_dev = blocks // groups
    tile = 2 * SUBLANES
    _, _, slots = energy_slots((tile, LANES), layer_dev)
    energy = x_ref[0, all_rows - tile :, :].astype(jnp.float32)
    for group in range(1, groups):
        energy += x_ref[group, all_rows - tile :, :].astype(jnp.float32)
    energy = jnp.sum(jnp.where(slots, energy, 0.0), axis=1, keepdims=True)
    scale = 1.0 / jnp.sqrt(energy[:layer_dev] / count + 1.0)
    scale = jnp.concatenate([scale] * (block_rows // layer_dev), axis=0)
    for group in range(groups):
        for block in range(blocks_dev):
            owner = owners_ref[group * blocks_dev + block]
            for part in range(strips):
                for piece in range(0, block_rows, tile):
                    start = part * rows + block * block_rows + piece
                    rest = x_ref[group, half + start : half + start + tile, :].astype(jnp.float32)
                    if start == half - tile:
                        rest = jnp.where(slots, 0.0, rest)
                    value = x_ref[group, start : start + tile, :].astype(jnp.float32) + rest
                    value = value * scale[piece : piece + tile]
                    place = part * block_rows + piece
                    out_ref[owner, place : place + tile, :] = value.astype(jnp.bfloat16)


def merge_kernel(layer_dev, x_ref, out_ref):
    block_len, layers, features = out_ref.shape
    devices, message_rows, _ = x_ref.shape
    block_rows = block_len * layer_dev
    strips = message_rows // block_rows
    sections = layers // layer_dev
    groups = devices // sections
    for group in range(groups):
        for part in range(strips):
            column = (group * strips + part) * LANES
            for token in range(block_len):
                start = part * block_rows + token * layer_dev
                value = jnp.concatenate(
                    [
                        x_ref[section * groups + group, start : start + layer_dev, :]
                        for section in range(sections)
                    ],
                    axis=0,
                )
                out_ref[token, :, column : column + LANES] = value


def on_device(residuals, owners):
    layer_dev, tok_dev, features = residuals.shape
    groups = lax.axis_size("dp")
    sections = lax.axis_size("section")
    blocks = owners.shape[0]
    block_len = tok_dev * groups // blocks
    strips = features // groups // LANES
    half = strips * tok_dev * layer_dev
    block_rows = block_len * layer_dev
    message = pl.pallas_call(
        spread_kernel,
        out_shape=jax.ShapeDtypeStruct((groups, 2 * half, LANES), jnp.bfloat16),
        scratch_shapes=[pltpu.VMEM((groups * half, LANES), jnp.float32)],
        compiler_params=LOCAL,
        name="spread",
    )(residuals)
    spread = lax.all_to_all(message, "dp", split_axis=0, concat_axis=0, tiled=True)
    count = float(tok_dev * groups * features)
    routed = pl.pallas_call(
        lambda *refs: route_kernel(count, layer_dev, block_rows, *refs),
        out_shape=jax.ShapeDtypeStruct((blocks, strips * block_rows, LANES), jnp.bfloat16),
        in_specs=[
            pl.BlockSpec(memory_space=pltpu.SMEM),
            pl.BlockSpec(memory_space=pltpu.VMEM),
        ],
        compiler_params=LOCAL,
        name="route",
    )(owners, spread)
    received = lax.all_to_all(routed, ("section", "dp"), split_axis=0, concat_axis=0, tiled=True)
    return pl.pallas_call(
        lambda *refs: merge_kernel(layer_dev, *refs),
        out_shape=jax.ShapeDtypeStruct((block_len, layer_dev * sections, features), jnp.bfloat16),
        compiler_params=LOCAL,
        name="merge",
    )(received)


def solution(mesh):
    in_specs = (P("section", "dp", None), P())
    out_specs = P(("section", "dp"), None, None)
    return jax.shard_map(
        on_device, mesh=mesh, in_specs=in_specs, out_specs=out_specs, check_vma=False
    )
```

```python
import jax
import jax.numpy as jnp
from jax import lax
from jax.experimental import pallas as pl
from jax.experimental.pallas import tpu as pltpu
from jax.sharding import PartitionSpec as P

LANES = 128
SUBLANES = 8
PARTS = 3
LOCAL = pltpu.CompilerParams(vmem_limit_bytes=16 * 1024 * 1024)


def ring_order(groups):
    return [(groups * 3 // 4 - 1 - place) % groups for place in range(groups)]


def split(value):
    high = value.astype(jnp.bfloat16)
    return high, value - high.astype(jnp.float32)


def energy_slots(shape, layer_dev):
    row = lax.broadcasted_iota(jnp.int32, shape, 0)
    lane = lax.broadcasted_iota(jnp.int32, shape, 1)
    return row, lane, (row < layer_dev) & (lane < PARTS)


def spread_kernel(x_ref, out_ref, rows_ref):
    layer_dev, tok_dev, features = x_ref.shape
    groups, all_rows, _ = out_ref.shape
    strips = features // groups // LANES
    rows = tok_dev * layer_dev
    half = all_rows // 2
    tile = 2 * SUBLANES
    row, lane, slots = energy_slots((tile, LANES), layer_dev)
    energy = jnp.zeros((tile, LANES), jnp.float32)
    for layer in range(layer_dev):
        value = x_ref[layer]
        centered = value - jnp.mean(value, axis=1, keepdims=True)
        energy = jnp.where(row == layer, jnp.sum(centered * centered), energy)
        for strip in range(groups * strips):
            rows_ref[pl.ds(strip * rows + layer, tok_dev, stride=layer_dev), :] = centered[
                :, strip * LANES : (strip + 1) * LANES
            ]
    first, rest = split(energy)
    second, rest = split(rest)
    energy = jnp.where(lane == 0, first.astype(jnp.float32), jnp.where(lane == 1, second.astype(jnp.float32), rest))
    for group in range(groups):
        for start in range(0, half, tile):
            high, rest = split(rows_ref[group * half + start : group * half + start + tile, :])
            if start == half - tile:
                rest = jnp.where(slots, energy, rest)
            out_ref[group, start : start + tile, :] = high
            out_ref[group, half + start : half + start + tile, :] = rest.astype(jnp.bfloat16)


def route_kernel(order, count, layer_dev, block_rows, owners_ref, x_ref, out_ref):
    groups, all_rows, _ = x_ref.shape
    blocks, message_rows, _ = out_ref.shape
    strips = message_rows // block_rows
    half = all_rows // 2
    rows = half // strips
    blocks_dev = blocks // groups
    tile = 2 * SUBLANES
    _, _, slots = energy_slots((tile, LANES), layer_dev)
    energy = x_ref[0, all_rows - tile :, :].astype(jnp.float32)
    for group in range(1, groups):
        energy += x_ref[group, all_rows - tile :, :].astype(jnp.float32)
    energy = jnp.sum(jnp.where(slots, energy, 0.0), axis=1, keepdims=True)
    scale = 1.0 / jnp.sqrt(energy[:layer_dev] / count + 1.0)
    scale = jnp.concatenate([scale] * (block_rows // layer_dev), axis=0)
    for group in range(groups):
        for block in range(blocks_dev):
            owner = owners_ref[order[group] * blocks_dev + block]
            for part in range(strips):
                for piece in range(0, block_rows, tile):
                    start = part * rows + block * block_rows + piece
                    rest = x_ref[group, half + start : half + start + tile, :].astype(jnp.float32)
                    if start == half - tile:
                        rest = jnp.where(slots, 0.0, rest)
                    value = x_ref[group, start : start + tile, :].astype(jnp.float32) + rest
                    value = value * scale[piece : piece + tile]
                    place = part * block_rows + piece
                    out_ref[owner, place : place + tile, :] = value.astype(jnp.bfloat16)


def merge_kernel(order, layer_dev, x_ref, out_ref):
    block_len, layers, features = out_ref.shape
    devices, message_rows, _ = x_ref.shape
    block_rows = block_len * layer_dev
    strips = message_rows // block_rows
    sections = layers // layer_dev
    groups = devices // sections
    for group in range(groups):
        for part in range(strips):
            column = (group * strips + part) * LANES
            for token in range(block_len):
                start = part * block_rows + token * layer_dev
                value = jnp.concatenate(
                    [
                        x_ref[section * groups + order[group], start : start + layer_dev, :]
                        for section in range(sections)
                    ],
                    axis=0,
                )
                out_ref[token, :, column : column + LANES] = value


def on_device(residuals, owners):
    layer_dev, tok_dev, features = residuals.shape
    groups = lax.axis_size("dp")
    sections = lax.axis_size("section")
    blocks = owners.shape[0]
    block_len = tok_dev * groups // blocks
    strips = features // groups // LANES
    half = strips * tok_dev * layer_dev
    order = ring_order(groups)
    block_rows = block_len * layer_dev
    message = pl.pallas_call(
        spread_kernel,
        out_shape=jax.ShapeDtypeStruct((groups, 2 * half, LANES), jnp.bfloat16),
        scratch_shapes=[pltpu.VMEM((groups * half, LANES), jnp.float32)],
        compiler_params=LOCAL,
        name="spread",
    )(residuals)
    spread = lax.all_to_all(
        message, "dp", split_axis=0, concat_axis=0, tiled=True, axis_index_groups=[order]
    )
    count = float(tok_dev * groups * features)
    routed = pl.pallas_call(
        lambda *refs: route_kernel(order, count, layer_dev, block_rows, *refs),
        out_shape=jax.ShapeDtypeStruct((blocks, strips * block_rows, LANES), jnp.bfloat16),
        in_specs=[
            pl.BlockSpec(memory_space=pltpu.SMEM),
            pl.BlockSpec(memory_space=pltpu.VMEM),
        ],
        compiler_params=LOCAL,
        name="route",
    )(owners, spread)
    received = lax.all_to_all(routed, ("section", "dp"), split_axis=0, concat_axis=0, tiled=True)
    return pl.pallas_call(
        lambda *refs: merge_kernel(order, layer_dev, *refs),
        out_shape=jax.ShapeDtypeStruct((block_len, layer_dev * sections, features), jnp.bfloat16),
        compiler_params=LOCAL,
        name="merge",
    )(received)


def solution(mesh):
    in_specs = (P("section", "dp", None), P())
    out_specs = P(("section", "dp"), None, None)
    return jax.shard_map(
        on_device, mesh=mesh, in_specs=in_specs, out_specs=out_specs, check_vma=False
    )
```

```python
import jax
import jax.numpy as jnp
from jax import lax
from jax.experimental import pallas as pl
from jax.experimental.pallas import tpu as pltpu
from jax.sharding import PartitionSpec as P

LANES = 128
SUBLANES = 8
PARTS = 3
LOCAL = pltpu.CompilerParams(vmem_limit_bytes=16 * 1024 * 1024)


def ring_order(groups):
    return [(groups * 3 // 4 - 1 - place) % groups for place in range(groups)]


def split(value):
    high = value.astype(jnp.bfloat16)
    return high, value - high.astype(jnp.float32)


def energy_slots(high, layer_dev):
    weight = high * high
    weight = weight[:SUBLANES] + weight[SUBLANES:]
    for shift in (4, 2, 1):
        weight += pltpu.roll(weight, shift, 0)
    lane = lax.broadcasted_iota(jnp.int32, weight.shape, 1).astype(jnp.float32)
    least = jnp.min(weight, axis=1, keepdims=True)
    first = jnp.min(jnp.where(weight == least, lane, float(LANES)), axis=1, keepdims=True)
    row = lax.broadcasted_iota(jnp.int32, high.shape, 0)
    chosen = jnp.concatenate([jnp.where(lane == first, 1.0, 0.0)] * 2, axis=0)
    return (chosen > 0.0) & (row < PARTS * layer_dev)


def spread_kernel(x_ref, out_ref, rows_ref):
    layer_dev, tok_dev, features = x_ref.shape
    groups, all_rows, _ = out_ref.shape
    strips = features // groups // LANES
    rows = tok_dev * layer_dev
    half = all_rows // 2
    tile = 2 * SUBLANES
    row = lax.broadcasted_iota(jnp.int32, (tile, LANES), 0)
    energy = jnp.zeros((tile, LANES), jnp.float32)
    for layer in range(layer_dev):
        value = x_ref[layer]
        centered = value - jnp.mean(value, axis=1, keepdims=True)
        energy = jnp.where(row % layer_dev == layer, jnp.sum(centered * centered), energy)
        for strip in range(groups * strips):
            rows_ref[pl.ds(strip * rows + layer, tok_dev, stride=layer_dev), :] = centered[
                :, strip * LANES : (strip + 1) * LANES
            ]
    first, rest = split(energy)
    second, rest = split(rest)
    energy = jnp.where(
        row < layer_dev,
        first.astype(jnp.float32),
        jnp.where(row < 2 * layer_dev, second.astype(jnp.float32), rest),
    )
    for group in range(groups):
        for start in range(0, half, tile):
            high, rest = split(rows_ref[group * half + start : group * half + start + tile, :])
            if start == half - tile:
                slots = energy_slots(high.astype(jnp.float32), layer_dev)
                rest = jnp.where(slots, energy, rest)
            out_ref[group, start : start + tile, :] = high
            out_ref[group, half + start : half + start + tile, :] = rest.astype(jnp.bfloat16)


def route_kernel(place_of, order, count, layer_dev, block_rows, owners_ref, x_ref, out_ref):
    groups, all_rows, _ = x_ref.shape
    blocks, message_rows, _ = out_ref.shape
    owners = owners_ref[...]
    strips = message_rows // block_rows
    half = all_rows // 2
    rows = half // strips
    blocks_dev = blocks // groups
    tile = 2 * SUBLANES
    energy = jnp.zeros((tile, LANES), jnp.float32)
    slots = []
    for group in range(groups):
        slots.append(energy_slots(x_ref[group, half - tile : half, :].astype(jnp.float32), layer_dev))
        rest = x_ref[group, all_rows - tile :, :].astype(jnp.float32)
        energy += jnp.where(slots[group], rest, 0.0)
    energy = jnp.sum(energy, axis=1, keepdims=True)
    energy = sum(energy[part * layer_dev : (part + 1) * layer_dev] for part in range(PARTS))
    scale = 1.0 / jnp.sqrt(energy / count + 1.0)
    scale = jnp.concatenate([scale] * (block_rows // layer_dev), axis=0)
    for group in range(groups):
        for block in range(blocks_dev):
            owner = place_of(owners[order[group] * blocks_dev + block])
            for part in range(strips):
                for piece in range(0, block_rows, tile):
                    start = part * rows + block * block_rows + piece
                    rest = x_ref[group, half + start : half + start + tile, :].astype(jnp.float32)
                    if start == half - tile:
                        rest = jnp.where(slots[group], 0.0, rest)
                    value = x_ref[group, start : start + tile, :].astype(jnp.float32) + rest
                    value = value * scale[piece : piece + tile]
                    place = part * block_rows + piece
                    out_ref[owner, place : place + tile, :] = value.astype(jnp.bfloat16)


def merge_kernel(place_of, order, layer_dev, x_ref, out_ref):
    block_len, layers, features = out_ref.shape
    devices, message_rows, _ = x_ref.shape
    block_rows = block_len * layer_dev
    strips = message_rows // block_rows
    sections = layers // layer_dev
    groups = devices // sections
    for group in range(groups):
        for part in range(strips):
            column = (group * strips + part) * LANES
            for token in range(block_len):
                start = part * block_rows + token * layer_dev
                value = jnp.concatenate(
                    [
                        x_ref[place_of(section * groups + order[group]), start : start + layer_dev, :]
                        for section in range(sections)
                    ],
                    axis=0,
                )
                out_ref[token, :, column : column + LANES] = value


def on_device(residuals, owners):
    layer_dev, tok_dev, features = residuals.shape
    groups = lax.axis_size("dp")
    sections = lax.axis_size("section")
    blocks = owners.shape[0]
    block_len = tok_dev * groups // blocks
    strips = features // groups // LANES
    half = strips * tok_dev * layer_dev
    order = ring_order(groups)

    def place_of(device):
        return (groups - 1 - device % groups) * sections + device // groups

    block_rows = block_len * layer_dev
    message = pl.pallas_call(
        spread_kernel,
        out_shape=jax.ShapeDtypeStruct((groups, 2 * half, LANES), jnp.bfloat16),
        scratch_shapes=[pltpu.VMEM((groups * half, LANES), jnp.float32)],
        compiler_params=LOCAL,
        name="spread",
    )(residuals)
    spread = lax.all_to_all(
        message, "dp", split_axis=0, concat_axis=0, tiled=True, axis_index_groups=[order]
    )
    count = float(tok_dev * groups * features)
    routed = pl.pallas_call(
        lambda *refs: route_kernel(place_of, order, count, layer_dev, block_rows, *refs),
        out_shape=jax.ShapeDtypeStruct((blocks, strips * block_rows, LANES), jnp.bfloat16),
        compiler_params=LOCAL,
        name="route",
    )(owners, spread)
    received = lax.all_to_all(
        routed,
        ("section", "dp"),
        split_axis=0,
        concat_axis=0,
        tiled=True,
        axis_index_groups=[sorted(range(blocks), key=place_of)],
    )
    return pl.pallas_call(
        lambda *refs: merge_kernel(place_of, order, layer_dev, *refs),
        out_shape=jax.ShapeDtypeStruct((block_len, layer_dev * sections, features), jnp.bfloat16),
        compiler_params=LOCAL,
        name="merge",
    )(received)


def solution(mesh):
    in_specs = (P("section", "dp", None), P())
    out_specs = P(("section", "dp"), None, None)
    return jax.shard_map(
        on_device, mesh=mesh, in_specs=in_specs, out_specs=out_specs, check_vma=False
    )
```

```python
import jax
import jax.numpy as jnp
from jax import lax
from jax.experimental import pallas as pl
from jax.experimental.pallas import tpu as pltpu
from jax.sharding import PartitionSpec as P

LANES = 128
SUBLANES = 8
PARTS = 3
LOCAL = pltpu.CompilerParams(vmem_limit_bytes=16 * 1024 * 1024)


def ring_order(groups):
    return [(groups * 3 // 4 - 1 - place) % groups for place in range(groups)]


def split(value):
    high = value.astype(jnp.bfloat16)
    return high, value - high.astype(jnp.float32)


def spare_lane(high):
    weight = high * high
    weight = weight[:SUBLANES] + weight[SUBLANES:]
    for shift in (4, 2, 1):
        weight += pltpu.roll(weight, shift, 0)
    lane = lax.broadcasted_iota(jnp.int32, weight.shape, 1)
    weight = jnp.where(lane == 0, jnp.inf, weight)
    least = jnp.min(weight, axis=1, keepdims=True)
    first = jnp.min(jnp.where(weight == least, lane.astype(jnp.float32), float(LANES)), axis=1, keepdims=True)
    return jnp.concatenate([first, first], axis=0)


def spread_kernel(x_ref, out_ref, rows_ref):
    layer_dev, tok_dev, features = x_ref.shape
    groups, all_rows, _ = out_ref.shape
    strips = features // groups // LANES
    rows = tok_dev * layer_dev
    half = all_rows // 2
    tile = 2 * SUBLANES
    row = lax.broadcasted_iota(jnp.int32, (tile, LANES), 0)
    lane = lax.broadcasted_iota(jnp.int32, (tile, LANES), 1)
    note = PARTS * layer_dev
    energy = jnp.zeros((tile, LANES), jnp.float32)
    for layer in range(layer_dev):
        value = x_ref[layer]
        centered = value - jnp.mean(value, axis=1, keepdims=True)
        energy = jnp.where(row % layer_dev == layer, jnp.sum(centered * centered), energy)
        for strip in range(groups * strips):
            rows_ref[pl.ds(strip * rows + layer, tok_dev, stride=layer_dev), :] = centered[
                :, strip * LANES : (strip + 1) * LANES
            ]
    first, rest = split(energy)
    second, rest = split(rest)
    energy = jnp.where(
        row < layer_dev,
        first.astype(jnp.float32),
        jnp.where(row < 2 * layer_dev, second.astype(jnp.float32), rest),
    )
    spares = []
    for group in range(groups):
        high, _ = split(rows_ref[(group + 1) * half - tile : (group + 1) * half, :])
        spares.append(spare_lane(high.astype(jnp.float32)))
    for group in range(groups):
        for start in range(0, half, tile):
            high, rest = split(rows_ref[group * half + start : group * half + start + tile, :])
            if start == half - tile:
                spare = spares[group]
                moved = (lane.astype(jnp.float32) == spare) & (row <= note)
                rest = jnp.where(moved, rest[:, :1], rest)
                fixed = jnp.where(row < note, energy, jnp.where(row == note, spare, rest))
                rest = jnp.where(lane == 0, fixed, rest)
            out_ref[group, start : start + tile, :] = high
            out_ref[group, half + start : half + start + tile, :] = rest.astype(jnp.bfloat16)


def route_kernel(place_of, order, count, layer_dev, block_rows, owners_ref, x_ref, out_ref):
    groups, all_rows, _ = x_ref.shape
    blocks, message_rows, _ = out_ref.shape
    owners = owners_ref[...]
    strips = message_rows // block_rows
    half = all_rows // 2
    rows = half // strips
    blocks_dev = blocks // groups
    tile = 2 * SUBLANES
    row = lax.broadcasted_iota(jnp.int32, (tile, LANES), 0)
    lane = lax.broadcasted_iota(jnp.int32, (tile, LANES), 1)
    note = PARTS * layer_dev
    energy = jnp.zeros((tile, LANES), jnp.float32)
    last = []
    for group in range(groups):
        rest = x_ref[group, all_rows - tile :, :].astype(jnp.float32)
        energy += rest
        moved = (lane.astype(jnp.float32) == rest[note : note + 1, :1]) & (row <= note)
        first = jnp.sum(jnp.where(moved, rest, 0.0), axis=1, keepdims=True)
        last.append(jnp.where(moved, 0.0, jnp.where((lane == 0) & (row <= note), first, rest)))
    energy = energy[:, :1]
    energy = sum(energy[part * layer_dev : (part + 1) * layer_dev] for part in range(PARTS))
    scale = 1.0 / jnp.sqrt(energy / count + 1.0)
    scale = jnp.concatenate([scale] * (block_rows // layer_dev), axis=0)
    for group in range(groups):
        for block in range(blocks_dev):
            owner = place_of(owners[order[group] * blocks_dev + block])
            for part in range(strips):
                for piece in range(0, block_rows, tile):
                    start = part * rows + block * block_rows + piece
                    if start == half - tile:
                        rest = last[group]
                    else:
                        rest = x_ref[group, half + start : half + start + tile, :].astype(jnp.float32)
                    value = x_ref[group, start : start + tile, :].astype(jnp.float32) + rest
                    value = value * scale[piece : piece + tile]
                    place = part * block_rows + piece
                    out_ref[owner, place : place + tile, :] = value.astype(jnp.bfloat16)


def merge_kernel(place_of, order, layer_dev, x_ref, out_ref):
    block_len, layers, features = out_ref.shape
    devices, message_rows, _ = x_ref.shape
    block_rows = block_len * layer_dev
    strips = message_rows // block_rows
    sections = layers // layer_dev
    groups = devices // sections
    for group in range(groups):
        for part in range(strips):
            column = (group * strips + part) * LANES
            for token in range(block_len):
                start = part * block_rows + token * layer_dev
                value = jnp.concatenate(
                    [
                        x_ref[place_of(section * groups + order[group]), start : start + layer_dev, :]
                        for section in range(sections)
                    ],
                    axis=0,
                )
                out_ref[token, :, column : column + LANES] = value


def on_device(residuals, owners):
    layer_dev, tok_dev, features = residuals.shape
    groups = lax.axis_size("dp")
    sections = lax.axis_size("section")
    blocks = owners.shape[0]
    block_len = tok_dev * groups // blocks
    strips = features // groups // LANES
    half = strips * tok_dev * layer_dev
    order = ring_order(groups)

    def place_of(device):
        return (groups - 1 - device % groups) * sections + device // groups

    block_rows = block_len * layer_dev
    message = pl.pallas_call(
        spread_kernel,
        out_shape=jax.ShapeDtypeStruct((groups, 2 * half, LANES), jnp.bfloat16),
        scratch_shapes=[pltpu.VMEM((groups * half, LANES), jnp.float32)],
        compiler_params=LOCAL,
        name="spread",
    )(residuals)
    spread = lax.all_to_all(
        message, "dp", split_axis=0, concat_axis=0, tiled=True, axis_index_groups=[order]
    )
    count = float(tok_dev * groups * features)
    routed = pl.pallas_call(
        lambda *refs: route_kernel(place_of, order, count, layer_dev, block_rows, *refs),
        out_shape=jax.ShapeDtypeStruct((blocks, strips * block_rows, LANES), jnp.bfloat16),
        compiler_params=LOCAL,
        name="route",
    )(owners, spread)
    received = lax.all_to_all(
        routed,
        ("section", "dp"),
        split_axis=0,
        concat_axis=0,
        tiled=True,
        axis_index_groups=[sorted(range(blocks), key=place_of)],
    )
    return pl.pallas_call(
        lambda *refs: merge_kernel(place_of, order, layer_dev, *refs),
        out_shape=jax.ShapeDtypeStruct((block_len, layer_dev * sections, features), jnp.bfloat16),
        compiler_params=LOCAL,
        name="merge",
    )(received)


def solution(mesh):
    in_specs = (P("section", "dp", None), P())
    out_specs = P(("section", "dp"), None, None)
    return jax.shard_map(
        on_device, mesh=mesh, in_specs=in_specs, out_specs=out_specs, check_vma=False
    )
```

```python
import jax
import jax.numpy as jnp
from jax import lax
from jax.experimental import pallas as pl
from jax.experimental.pallas import tpu as pltpu
from jax.sharding import PartitionSpec as P

LANES = 128
SUBLANES = 8
PARTS = 3
LOCAL = pltpu.CompilerParams(vmem_limit_bytes=16 * 1024 * 1024)


def ring_order(groups):
    return [(groups * 3 // 4 - 1 - place) % groups for place in range(groups)]


def split(value):
    high = value.astype(jnp.bfloat16)
    return high, value - high.astype(jnp.float32)


def spare_lane(weight):
    weight = weight[:SUBLANES] + weight[SUBLANES:]
    for shift in (4, 2, 1):
        weight += pltpu.roll(weight, shift, 0)
    lane = lax.broadcasted_iota(jnp.int32, weight.shape, 1)
    weight = jnp.where(lane == 0, jnp.inf, weight)
    least = jnp.min(weight, axis=1, keepdims=True)
    first = jnp.min(jnp.where(weight == least, lane.astype(jnp.float32), float(LANES)), axis=1, keepdims=True)
    return jnp.concatenate([first, first], axis=0)


def spread_kernel(x_ref, out_ref, rows_ref):
    layer_dev, tok_dev, features = x_ref.shape
    groups, all_rows, _ = out_ref.shape
    strips = features // groups // LANES
    rows = tok_dev * layer_dev
    half = all_rows // 2
    tile = 2 * SUBLANES
    row = lax.broadcasted_iota(jnp.int32, (tile, LANES), 0)
    lane = lax.broadcasted_iota(jnp.int32, (tile, LANES), 1)
    note = PARTS * layer_dev
    energy = jnp.zeros((tile, LANES), jnp.float32)
    for layer in range(layer_dev):
        value = x_ref[layer]
        centered = value - jnp.mean(value, axis=1, keepdims=True)
        energy = jnp.where(row % layer_dev == layer, jnp.sum(centered * centered), energy)
        for strip in range(groups * strips):
            rows_ref[pl.ds(strip * rows + layer, tok_dev, stride=layer_dev), :] = centered[
                :, strip * LANES : (strip + 1) * LANES
            ]
    first, rest = split(energy)
    second, rest = split(rest)
    energy = jnp.where(
        row < layer_dev,
        first.astype(jnp.float32),
        jnp.where(row < 2 * layer_dev, second.astype(jnp.float32), rest),
    )
    weight = jnp.zeros((tile, LANES), jnp.float32)
    for group in range(groups):
        value = rows_ref[(group + 1) * half - tile : (group + 1) * half, :]
        weight += value * value
    spare = spare_lane(weight)
    moved = (lane.astype(jnp.float32) == spare) & (row <= note)
    noted = jnp.where(row < note, energy, spare)
    for group in range(groups):
        for start in range(0, half, tile):
            high, rest = split(rows_ref[group * half + start : group * half + start + tile, :])
            if start == half - tile:
                rest = jnp.where(moved, rest[:, :1], rest)
                rest = jnp.where((lane == 0) & (row <= note), noted, rest)
            out_ref[group, start : start + tile, :] = high
            out_ref[group, half + start : half + start + tile, :] = rest.astype(jnp.bfloat16)


def route_kernel(place_of, order, count, layer_dev, block_rows, owners_ref, x_ref, out_ref):
    groups, all_rows, _ = x_ref.shape
    blocks, message_rows, _ = out_ref.shape
    owners = owners_ref[...]
    strips = message_rows // block_rows
    half = all_rows // 2
    rows = half // strips
    blocks_dev = blocks // groups
    tile = 2 * SUBLANES
    row = lax.broadcasted_iota(jnp.int32, (tile, LANES), 0)
    lane = lax.broadcasted_iota(jnp.int32, (tile, LANES), 1)
    note = PARTS * layer_dev
    energy = jnp.zeros((tile, LANES), jnp.float32)
    last = []
    for group in range(groups):
        rest = x_ref[group, all_rows - tile :, :].astype(jnp.float32)
        energy += rest
        moved = (lane.astype(jnp.float32) == rest[note : note + 1, :1]) & (row <= note)
        first = jnp.sum(jnp.where(moved, rest, 0.0), axis=1, keepdims=True)
        last.append(jnp.where(moved, 0.0, jnp.where((lane == 0) & (row <= note), first, rest)))
    energy = energy[:, :1]
    energy = sum(energy[part * layer_dev : (part + 1) * layer_dev] for part in range(PARTS))
    scale = 1.0 / jnp.sqrt(energy / count + 1.0)
    scale = jnp.concatenate([scale] * (block_rows // layer_dev), axis=0)
    for group in range(groups):
        for block in range(blocks_dev):
            owner = place_of(owners[order[group] * blocks_dev + block])
            for part in range(strips):
                for piece in range(0, block_rows, tile):
                    start = part * rows + block * block_rows + piece
                    if start == half - tile:
                        rest = last[group]
                    else:
                        rest = x_ref[group, half + start : half + start + tile, :].astype(jnp.float32)
                    value = x_ref[group, start : start + tile, :].astype(jnp.float32) + rest
                    value = value * scale[piece : piece + tile]
                    place = part * block_rows + piece
                    out_ref[owner, place : place + tile, :] = value.astype(jnp.bfloat16)


def merge_kernel(place_of, order, layer_dev, x_ref, out_ref):
    block_len, layers, features = out_ref.shape
    devices, message_rows, _ = x_ref.shape
    block_rows = block_len * layer_dev
    strips = message_rows // block_rows
    sections = layers // layer_dev
    groups = devices // sections
    for group in range(groups):
        for part in range(strips):
            column = (group * strips + part) * LANES
            for token in range(block_len):
                start = part * block_rows + token * layer_dev
                value = jnp.concatenate(
                    [
                        x_ref[place_of(section * groups + order[group]), start : start + layer_dev, :]
                        for section in range(sections)
                    ],
                    axis=0,
                )
                out_ref[token, :, column : column + LANES] = value


def on_device(residuals, owners):
    layer_dev, tok_dev, features = residuals.shape
    groups = lax.axis_size("dp")
    sections = lax.axis_size("section")
    blocks = owners.shape[0]
    block_len = tok_dev * groups // blocks
    strips = features // groups // LANES
    half = strips * tok_dev * layer_dev
    order = ring_order(groups)

    def place_of(device):
        return (groups - 1 - device % groups) * sections + device // groups

    block_rows = block_len * layer_dev
    message = pl.pallas_call(
        spread_kernel,
        out_shape=jax.ShapeDtypeStruct((groups, 2 * half, LANES), jnp.bfloat16),
        scratch_shapes=[pltpu.VMEM((groups * half, LANES), jnp.float32)],
        compiler_params=LOCAL,
        name="spread",
    )(residuals)
    spread = lax.all_to_all(
        message, "dp", split_axis=0, concat_axis=0, tiled=True, axis_index_groups=[order]
    )
    count = float(tok_dev * groups * features)
    routed = pl.pallas_call(
        lambda *refs: route_kernel(place_of, order, count, layer_dev, block_rows, *refs),
        out_shape=jax.ShapeDtypeStruct((blocks, strips * block_rows, LANES), jnp.bfloat16),
        compiler_params=LOCAL,
        name="route",
    )(owners, spread)
    received = lax.all_to_all(
        routed,
        ("section", "dp"),
        split_axis=0,
        concat_axis=0,
        tiled=True,
        axis_index_groups=[sorted(range(blocks), key=place_of)],
    )
    return pl.pallas_call(
        lambda *refs: merge_kernel(place_of, order, layer_dev, *refs),
        out_shape=jax.ShapeDtypeStruct((block_len, layer_dev * sections, features), jnp.bfloat16),
        compiler_params=LOCAL,
        name="merge",
    )(received)


def solution(mesh):
    in_specs = (P("section", "dp", None), P())
    out_specs = P(("section", "dp"), None, None)
    return jax.shard_map(
        on_device, mesh=mesh, in_specs=in_specs, out_specs=out_specs, check_vma=False
    )
```

```python
import jax
import jax.numpy as jnp
from jax import lax
from jax.experimental import pallas as pl
from jax.experimental.pallas import tpu as pltpu
from jax.sharding import PartitionSpec as P

LANES = 128
SUBLANES = 8
PARTS = 3
LOCAL = pltpu.CompilerParams(vmem_limit_bytes=16 * 1024 * 1024)


def ring_order(groups):
    return [(groups * 3 // 4 - 1 - place) % groups for place in range(groups)]


def split(value):
    high = value.astype(jnp.bfloat16)
    return high, value - high.astype(jnp.float32)


def spare_lane(weight):
    weight = weight[:SUBLANES] + weight[SUBLANES:]
    for shift in (4, 2, 1):
        weight += pltpu.roll(weight, shift, 0)
    lane = lax.broadcasted_iota(jnp.int32, weight.shape, 1)
    weight = jnp.where(lane == 0, jnp.inf, weight)
    least = jnp.min(weight, axis=1, keepdims=True)
    first = jnp.min(jnp.where(weight == least, lane.astype(jnp.float32), float(LANES)), axis=1, keepdims=True)
    return jnp.concatenate([first, first], axis=0)


def spread_kernel(x_ref, out_ref, rows_ref):
    layer_dev, tok_dev, features = x_ref.shape
    groups, all_rows, _ = out_ref.shape
    strips = features // groups // LANES
    rows = tok_dev * layer_dev
    half = all_rows // 2
    tile = 2 * SUBLANES
    row = lax.broadcasted_iota(jnp.int32, (tile, LANES), 0)
    lane = lax.broadcasted_iota(jnp.int32, (tile, LANES), 1)
    note = PARTS * layer_dev
    energy = jnp.zeros((tile, LANES), jnp.float32)
    for layer in range(layer_dev):
        value = x_ref[layer]
        centered = value - jnp.mean(value, axis=1, keepdims=True)
        energy = jnp.where(row % layer_dev == layer, jnp.sum(centered * centered), energy)
        for strip in range(groups * strips):
            rows_ref[pl.ds(strip * rows + layer, tok_dev, stride=layer_dev), :] = centered[
                :, strip * LANES : (strip + 1) * LANES
            ]
    first, rest = split(energy)
    second, rest = split(rest)
    energy = jnp.where(
        row < layer_dev,
        first.astype(jnp.float32),
        jnp.where(row < 2 * layer_dev, second.astype(jnp.float32), rest),
    )
    weight = jnp.zeros((tile, LANES), jnp.float32)
    for group in range(groups):
        value = rows_ref[(group + 1) * half - tile : (group + 1) * half, :]
        weight += value * value
    spare = spare_lane(weight)
    moved = (lane.astype(jnp.float32) == spare) & (row <= note)
    noted = jnp.where(row < note, energy, spare)
    for group in range(groups):
        for start in range(0, half, tile):
            high, rest = split(rows_ref[group * half + start : group * half + start + tile, :])
            if start == half - tile:
                rest = jnp.where(moved, rest[:, :1], rest)
                rest = jnp.where((lane == 0) & (row <= note), noted, rest)
            out_ref[group, start : start + tile, :] = high
            out_ref[group, half + start : half + start + tile, :] = rest.astype(jnp.bfloat16)


def route_kernel(place_of, order, count, layer_dev, block_rows, owners_ref, x_ref, out_ref):
    groups, all_rows, _ = x_ref.shape
    blocks, message_rows, _ = out_ref.shape
    owners = owners_ref[...]
    strips = message_rows // block_rows
    half = all_rows // 2
    rows = half // strips
    blocks_dev = blocks // groups
    tile = 2 * SUBLANES
    row = lax.broadcasted_iota(jnp.int32, (tile, LANES), 0)
    lane = lax.broadcasted_iota(jnp.int32, (tile, LANES), 1)
    note = PARTS * layer_dev
    energy = jnp.zeros((tile, LANES), jnp.float32)
    last = []
    for group in range(groups):
        rest = x_ref[group, all_rows - tile :, :].astype(jnp.float32)
        energy += rest
        moved = (lane.astype(jnp.float32) == rest[note : note + 1, :1]) & (row <= note)
        first = jnp.sum(jnp.where(moved, rest, 0.0), axis=1, keepdims=True)
        last.append(jnp.where(moved, 0.0, jnp.where((lane == 0) & (row <= note), first, rest)))
    energy = energy[:, :1]
    energy = sum(energy[part * layer_dev : (part + 1) * layer_dev] for part in range(PARTS))
    scale = 1.0 / jnp.sqrt(energy / count + 1.0)
    scale = jnp.concatenate([scale] * (block_rows // layer_dev), axis=0)
    for group in range(groups):
        for block in range(blocks_dev):
            owner = place_of(owners[order[group] * blocks_dev + block])
            for part in range(strips):
                for piece in range(0, block_rows, tile):
                    start = part * rows + block * block_rows + piece
                    if start == half - tile:
                        rest = last[group]
                    else:
                        rest = x_ref[group, half + start : half + start + tile, :].astype(jnp.float32)
                    value = x_ref[group, start : start + tile, :].astype(jnp.float32) + rest
                    value = value * scale[piece : piece + tile]
                    place = part * block_rows + piece
                    out_ref[owner, place : place + tile, :] = value.astype(jnp.bfloat16)


def merge_kernel(place_of, order, layer_dev, x_ref, out_ref, near_ref, sems):
    block_len, layers, features = out_ref.shape
    devices, message_rows, _ = x_ref.shape
    block_rows = block_len * layer_dev
    strips = message_rows // block_rows
    sections = layers // layer_dev
    groups = devices // sections
    stores = []
    for token in range(block_len):
        for group in range(groups):
            for part in range(strips):
                column = (group * strips + part) * LANES
                start = part * block_rows + token * layer_dev
                value = jnp.concatenate(
                    [
                        x_ref[place_of(section * groups + order[group]), start : start + layer_dev, :]
                        for section in range(sections)
                    ],
                    axis=0,
                )
                near_ref[token, :, column : column + LANES] = value
        store = pltpu.make_async_copy(near_ref.at[token], out_ref.at[token], sems.at[token])
        store.start()
        stores.append(store)
    for store in stores:
        store.wait()


def on_device(residuals, owners):
    layer_dev, tok_dev, features = residuals.shape
    groups = lax.axis_size("dp")
    sections = lax.axis_size("section")
    blocks = owners.shape[0]
    block_len = tok_dev * groups // blocks
    strips = features // groups // LANES
    half = strips * tok_dev * layer_dev
    order = ring_order(groups)

    def place_of(device):
        index = device % groups
        return (index ^ 3 if groups % 4 == 0 else index) * sections + device // groups

    block_rows = block_len * layer_dev
    message = pl.pallas_call(
        spread_kernel,
        out_shape=jax.ShapeDtypeStruct((groups, 2 * half, LANES), jnp.bfloat16),
        scratch_shapes=[pltpu.VMEM((groups * half, LANES), jnp.float32)],
        compiler_params=LOCAL,
        name="spread",
    )(residuals)
    spread = lax.all_to_all(
        message, "dp", split_axis=0, concat_axis=0, tiled=True, axis_index_groups=[order]
    )
    count = float(tok_dev * groups * features)
    routed = pl.pallas_call(
        lambda *refs: route_kernel(place_of, order, count, layer_dev, block_rows, *refs),
        out_shape=jax.ShapeDtypeStruct((blocks, strips * block_rows, LANES), jnp.bfloat16),
        compiler_params=LOCAL,
        name="route",
    )(owners, spread)
    received = lax.all_to_all(
        routed,
        ("section", "dp"),
        split_axis=0,
        concat_axis=0,
        tiled=True,
        axis_index_groups=[sorted(range(blocks), key=place_of)],
    )
    return pl.pallas_call(
        lambda *refs: merge_kernel(place_of, order, layer_dev, *refs),
        out_shape=jax.ShapeDtypeStruct((block_len, layer_dev * sections, features), jnp.bfloat16),
        out_specs=pl.BlockSpec(memory_space=pltpu.HBM),
        scratch_shapes=[
            pltpu.VMEM((block_len, layer_dev * sections, features), jnp.bfloat16),
            pltpu.SemaphoreType.DMA((block_len,)),
        ],
        compiler_params=LOCAL,
        name="merge",
    )(received)


def solution(mesh):
    in_specs = (P("section", "dp", None), P())
    out_specs = P(("section", "dp"), None, None)
    return jax.shard_map(
        on_device, mesh=mesh, in_specs=in_specs, out_specs=out_specs, check_vma=False
    )
```

```python
import jax
import jax.numpy as jnp
from jax import lax
from jax.experimental import pallas as pl
from jax.experimental.pallas import tpu as pltpu
from jax.sharding import PartitionSpec as P

LANES = 128
SUBLANES = 8
PARTS = 3
LOCAL = pltpu.CompilerParams(vmem_limit_bytes=16 * 1024 * 1024)


def ring_order(groups):
    return [(groups * 3 // 4 - 1 - place) % groups for place in range(groups)]


def split(value):
    high = value.astype(jnp.bfloat16)
    return high, value - high.astype(jnp.float32)


def spare_lane(weight):
    weight = weight[:SUBLANES] + weight[SUBLANES:]
    for shift in (4, 2, 1):
        weight += pltpu.roll(weight, shift, 0)
    lane = lax.broadcasted_iota(jnp.int32, weight.shape, 1)
    weight = jnp.where(lane == 0, jnp.inf, weight)
    first = jnp.argmin(weight, axis=1, keepdims=True).astype(jnp.float32)
    return jnp.concatenate([first, first], axis=0)


def spread_kernel(x_ref, out_ref, rows_ref):
    layer_dev, tok_dev, features = x_ref.shape
    groups, all_rows, _ = out_ref.shape
    strips = features // groups // LANES
    rows = tok_dev * layer_dev
    half = all_rows // 2
    tile = 2 * SUBLANES
    row = lax.broadcasted_iota(jnp.int32, (tile, LANES), 0)
    lane = lax.broadcasted_iota(jnp.int32, (tile, LANES), 1)
    note = PARTS * layer_dev
    energy = jnp.zeros((tile, LANES), jnp.float32)
    for layer in range(layer_dev):
        value = x_ref[layer]
        centered = value - jnp.mean(value, axis=1, keepdims=True)
        energy = jnp.where(row % layer_dev == layer, jnp.sum(centered * centered), energy)
        for strip in range(groups * strips):
            rows_ref[pl.ds(strip * rows + layer, tok_dev, stride=layer_dev), :] = centered[
                :, strip * LANES : (strip + 1) * LANES
            ]
    first, rest = split(energy)
    second, rest = split(rest)
    energy = jnp.where(
        row < layer_dev,
        first.astype(jnp.float32),
        jnp.where(row < 2 * layer_dev, second.astype(jnp.float32), rest),
    )
    weight = jnp.zeros((tile, LANES), jnp.float32)
    for group in range(groups):
        value = rows_ref[(group + 1) * half - tile : (group + 1) * half, :]
        weight += value * value
    spare = spare_lane(weight)
    moved = (lane.astype(jnp.float32) == spare) & (row <= note)
    noted = jnp.where(row < note, energy, spare)
    for group in range(groups):
        for start in range(0, half, tile):
            high, rest = split(rows_ref[group * half + start : group * half + start + tile, :])
            if start == half - tile:
                rest = jnp.where(moved, rest[:, :1], rest)
                rest = jnp.where((lane == 0) & (row <= note), noted, rest)
            out_ref[group, start : start + tile, :] = high
            out_ref[group, half + start : half + start + tile, :] = rest.astype(jnp.bfloat16)


def route_kernel(place_of, order, count, layer_dev, block_rows, owners_ref, x_ref, out_ref):
    groups, all_rows, _ = x_ref.shape
    blocks, message_rows, _ = out_ref.shape
    owners = owners_ref[...]
    strips = message_rows // block_rows
    half = all_rows // 2
    rows = half // strips
    blocks_dev = blocks // groups
    tile = 2 * SUBLANES
    row = lax.broadcasted_iota(jnp.int32, (tile, LANES), 0)
    lane = lax.broadcasted_iota(jnp.int32, (tile, LANES), 1)
    note = PARTS * layer_dev
    energy = jnp.zeros((tile, LANES), jnp.float32)
    last = []
    for group in range(groups):
        rest = x_ref[group, all_rows - tile :, :].astype(jnp.float32)
        energy += rest
        moved = (lane.astype(jnp.float32) == rest[note : note + 1, :1]) & (row <= note)
        first = jnp.sum(jnp.where(moved, rest, 0.0), axis=1, keepdims=True)
        last.append(jnp.where(moved, 0.0, jnp.where((lane == 0) & (row <= note), first, rest)))
    energy = energy[:, :1]
    energy = sum(energy[part * layer_dev : (part + 1) * layer_dev] for part in range(PARTS))
    scale = 1.0 / jnp.sqrt(energy / count + 1.0)
    scale = jnp.concatenate([scale] * (block_rows // layer_dev), axis=0)
    for group in range(groups):
        for block in range(blocks_dev):
            owner = place_of(owners[order[group] * blocks_dev + block])
            for part in range(strips):
                for piece in range(0, block_rows, tile):
                    start = part * rows + block * block_rows + piece
                    if start == half - tile:
                        rest = last[group]
                    else:
                        rest = x_ref[group, half + start : half + start + tile, :].astype(jnp.float32)
                    value = x_ref[group, start : start + tile, :].astype(jnp.float32) + rest
                    value = value * scale[piece : piece + tile]
                    place = part * block_rows + piece
                    out_ref[owner, place : place + tile, :] = value.astype(jnp.bfloat16)


def merge_kernel(place_of, order, layer_dev, x_ref, out_ref, near_ref, sems):
    block_len, layers, features = out_ref.shape
    devices, message_rows, _ = x_ref.shape
    block_rows = block_len * layer_dev
    strips = message_rows // block_rows
    sections = layers // layer_dev
    groups = devices // sections
    stores = []
    for token in range(block_len):
        for group in range(groups):
            for part in range(strips):
                column = (group * strips + part) * LANES
                start = part * block_rows + token * layer_dev
                value = jnp.concatenate(
                    [
                        x_ref[place_of(section * groups + order[group]), start : start + layer_dev, :]
                        for section in range(sections)
                    ],
                    axis=0,
                )
                near_ref[token, :, column : column + LANES] = value
        store = pltpu.make_async_copy(near_ref.at[token], out_ref.at[token], sems.at[token])
        store.start()
        stores.append(store)
    for store in stores:
        store.wait()


def on_device(residuals, owners):
    layer_dev, tok_dev, features = residuals.shape
    groups = lax.axis_size("dp")
    sections = lax.axis_size("section")
    blocks = owners.shape[0]
    block_len = tok_dev * groups // blocks
    strips = features // groups // LANES
    half = strips * tok_dev * layer_dev
    order = ring_order(groups)

    def place_of(device):
        index = device % groups
        return (index ^ 3 if groups % 4 == 0 else index) * sections + device // groups

    block_rows = block_len * layer_dev
    message = pl.pallas_call(
        spread_kernel,
        out_shape=jax.ShapeDtypeStruct((groups, 2 * half, LANES), jnp.bfloat16),
        scratch_shapes=[pltpu.VMEM((groups * half, LANES), jnp.float32)],
        compiler_params=LOCAL,
        name="spread",
    )(residuals)
    spread = lax.all_to_all(
        message, "dp", split_axis=0, concat_axis=0, tiled=True, axis_index_groups=[order]
    )
    count = float(tok_dev * groups * features)
    routed = pl.pallas_call(
        lambda *refs: route_kernel(place_of, order, count, layer_dev, block_rows, *refs),
        out_shape=jax.ShapeDtypeStruct((blocks, strips * block_rows, LANES), jnp.bfloat16),
        compiler_params=LOCAL,
        name="route",
    )(owners, spread)
    received = lax.all_to_all(
        routed,
        ("section", "dp"),
        split_axis=0,
        concat_axis=0,
        tiled=True,
        axis_index_groups=[sorted(range(blocks), key=place_of)],
    )
    return pl.pallas_call(
        lambda *refs: merge_kernel(place_of, order, layer_dev, *refs),
        out_shape=jax.ShapeDtypeStruct((block_len, layer_dev * sections, features), jnp.bfloat16),
        out_specs=pl.BlockSpec(memory_space=pltpu.HBM),
        scratch_shapes=[
            pltpu.VMEM((block_len, layer_dev * sections, features), jnp.bfloat16),
            pltpu.SemaphoreType.DMA((block_len,)),
        ],
        compiler_params=LOCAL,
        name="merge",
    )(received)


def solution(mesh):
    in_specs = (P("section", "dp", None), P())
    out_specs = P(("section", "dp"), None, None)
    return jax.shard_map(
        on_device, mesh=mesh, in_specs=in_specs, out_specs=out_specs, check_vma=False
    )
```

```python
import jax
import jax.numpy as jnp
from jax import lax
from jax.experimental import pallas as pl
from jax.experimental.pallas import tpu as pltpu
from jax.sharding import PartitionSpec as P

LANES = 128
SUBLANES = 8
PARTS = 3
LOCAL = pltpu.CompilerParams(vmem_limit_bytes=16 * 1024 * 1024)


def ring_order(groups):
    return [(groups * 3 // 4 - 1 - place) % groups for place in range(groups)]


def split(value):
    high = value.astype(jnp.bfloat16)
    return high, value - high.astype(jnp.float32)


def spare_lane(weight):
    weight = weight[:SUBLANES] + weight[SUBLANES:]
    for shift in (4, 2, 1):
        weight += pltpu.roll(weight, shift, 0)
    lane = lax.broadcasted_iota(jnp.int32, weight.shape, 1)
    weight = jnp.where(lane == 0, jnp.inf, weight)
    first = jnp.argmin(weight, axis=1, keepdims=True).astype(jnp.float32)
    return jnp.concatenate([first, first], axis=0)


def spread_kernel(x_ref, out_ref, rows_ref):
    layer_dev, tok_dev, features = x_ref.shape
    groups, all_rows, _ = out_ref.shape
    strips = features // groups // LANES
    rows = tok_dev * layer_dev
    half = all_rows // 2
    tile = 2 * SUBLANES
    row = lax.broadcasted_iota(jnp.int32, (tile, LANES), 0)
    lane = lax.broadcasted_iota(jnp.int32, (tile, LANES), 1)
    note = PARTS * layer_dev
    energy = jnp.zeros((tile, LANES), jnp.float32)
    for layer in range(layer_dev):
        value = x_ref[layer]
        centered = value - jnp.mean(value, axis=1, keepdims=True)
        energy = jnp.where(row % layer_dev == layer, jnp.sum(centered * centered), energy)
        for strip in range(groups * strips):
            rows_ref[pl.ds(strip * rows + layer, tok_dev, stride=layer_dev), :] = centered[
                :, strip * LANES : (strip + 1) * LANES
            ]
    first, rest = split(energy)
    second, rest = split(rest)
    energy = jnp.where(
        row < layer_dev,
        first.astype(jnp.float32),
        jnp.where(row < 2 * layer_dev, second.astype(jnp.float32), rest),
    )
    weight = jnp.zeros((tile, LANES), jnp.float32)
    for group in range(groups):
        value = rows_ref[(group + 1) * half - tile : (group + 1) * half, :]
        weight += value * value
    spare = spare_lane(weight)
    moved = (lane.astype(jnp.float32) == spare) & (row <= note)
    noted = jnp.where(row < note, energy, spare)
    for group in range(groups):
        for start in range(0, half, tile):
            high, rest = split(rows_ref[group * half + start : group * half + start + tile, :])
            if start == half - tile:
                rest = jnp.where(moved, rest[:, :1], rest)
                rest = jnp.where((lane == 0) & (row <= note), noted, rest)
            out_ref[group, start : start + tile, :] = high
            out_ref[group, half + start : half + start + tile, :] = rest.astype(jnp.bfloat16)


def route_kernel(place_of, order, count, layer_dev, block_rows, owners_ref, x_ref, out_ref):
    groups, all_rows, _ = x_ref.shape
    blocks, message_rows, _ = out_ref.shape
    owners = owners_ref[...]
    strips = message_rows // block_rows
    half = all_rows // 2
    rows = half // strips
    blocks_dev = blocks // groups
    tile = 2 * SUBLANES
    row = lax.broadcasted_iota(jnp.int32, (tile, LANES), 0)
    lane = lax.broadcasted_iota(jnp.int32, (tile, LANES), 1)
    note = PARTS * layer_dev
    energy = jnp.zeros((tile, LANES), jnp.float32)
    last = []
    for group in range(groups):
        rest = x_ref[group, all_rows - tile :, :].astype(jnp.float32)
        energy += rest
        moved = (lane.astype(jnp.float32) == rest[note : note + 1, :1]) & (row <= note)
        first = jnp.sum(jnp.where(moved, rest, 0.0), axis=1, keepdims=True)
        last.append(jnp.where(moved, 0.0, jnp.where((lane == 0) & (row <= note), first, rest)))
    energy = energy[:, :1]
    energy = sum(energy[part * layer_dev : (part + 1) * layer_dev] for part in range(PARTS))
    scale = 1.0 / jnp.sqrt(energy / count + 1.0)
    scale = jnp.concatenate([scale] * (block_rows // layer_dev), axis=0)
    for group in range(groups):
        for block in range(blocks_dev):
            owner = place_of(owners[order[group] * blocks_dev + block])
            for part in range(strips):
                for piece in range(0, block_rows, tile):
                    start = part * rows + block * block_rows + piece
                    if start == half - tile:
                        rest = last[group]
                    else:
                        rest = x_ref[group, half + start : half + start + tile, :].astype(jnp.float32)
                    value = x_ref[group, start : start + tile, :].astype(jnp.float32) + rest
                    value = value * scale[piece : piece + tile]
                    place = part * block_rows + piece
                    out_ref[owner, place : place + tile, :] = value.astype(jnp.bfloat16)


def merge_kernel(place_of, order, layer_dev, x_ref, out_ref, near_ref, sems):
    block_len, layers, features = out_ref.shape
    devices, message_rows, _ = x_ref.shape
    block_rows = block_len * layer_dev
    strips = message_rows // block_rows
    sections = layers // layer_dev
    groups = devices // sections
    stores = []
    for token in range(block_len):
        for group in range(groups):
            for part in range(strips):
                column = (group * strips + part) * LANES
                start = part * block_rows + token * layer_dev
                value = jnp.concatenate(
                    [
                        x_ref[place_of(section * groups + order[group]), start : start + layer_dev, :]
                        for section in range(sections)
                    ],
                    axis=0,
                )
                near_ref[token, :, column : column + LANES] = value
        store = pltpu.make_async_copy(near_ref.at[token], out_ref.at[token], sems.at[token])
        store.start()
        stores.append(store)
    for store in stores:
        store.wait()


def on_device(residuals, owners):
    layer_dev, tok_dev, features = residuals.shape
    groups = lax.axis_size("dp")
    sections = lax.axis_size("section")
    blocks = owners.shape[0]
    block_len = tok_dev * groups // blocks
    strips = features // groups // LANES
    half = strips * tok_dev * layer_dev
    order = ring_order(groups)

    def place_of(device):
        index = device % groups
        return (groups - 1 - index) * sections + device // groups

    block_rows = block_len * layer_dev
    message = pl.pallas_call(
        spread_kernel,
        out_shape=jax.ShapeDtypeStruct((groups, 2 * half, LANES), jnp.bfloat16),
        scratch_shapes=[pltpu.VMEM((groups * half, LANES), jnp.float32)],
        compiler_params=LOCAL,
        name="spread",
    )(residuals)
    spread = lax.all_to_all(
        message, "dp", split_axis=0, concat_axis=0, tiled=True, axis_index_groups=[order]
    )
    count = float(tok_dev * groups * features)
    routed = pl.pallas_call(
        lambda *refs: route_kernel(place_of, order, count, layer_dev, block_rows, *refs),
        out_shape=jax.ShapeDtypeStruct((blocks, strips * block_rows, LANES), jnp.bfloat16),
        compiler_params=LOCAL,
        name="route",
    )(owners, spread)
    received = lax.all_to_all(
        routed,
        ("section", "dp"),
        split_axis=0,
        concat_axis=0,
        tiled=True,
        axis_index_groups=[sorted(range(blocks), key=place_of)],
    )
    return pl.pallas_call(
        lambda *refs: merge_kernel(place_of, order, layer_dev, *refs),
        out_shape=jax.ShapeDtypeStruct((block_len, layer_dev * sections, features), jnp.bfloat16),
        out_specs=pl.BlockSpec(memory_space=pltpu.HBM),
        scratch_shapes=[
            pltpu.VMEM((block_len, layer_dev * sections, features), jnp.bfloat16),
            pltpu.SemaphoreType.DMA((block_len,)),
        ],
        compiler_params=LOCAL,
        name="merge",
    )(received)


def solution(mesh):
    in_specs = (P("section", "dp", None), P())
    out_specs = P(("section", "dp"), None, None)
    return jax.shard_map(
        on_device, mesh=mesh, in_specs=in_specs, out_specs=out_specs, check_vma=False
    )
```
